256 devices in a mesh: group: 64 (over z, x, core), peer: 4 (over y).
Axes of the slice: x: 4, y: 4, z: 8, core: 2. Of those that a mesh axis runs over, the one named last changes fastest.
Arguments:
- features: bfloat16 [98304, 1024], P(('group', 'peer')), may hold values from -6 to 6
- task_mask: int32 [98304], P(('group', 'peer')), may hold values from 0 to 65535, as said below
- tower_in: bfloat16 [16, 2048, 1024], P('peer', 'group'), may hold values from -0.1875 to 0.1875
- tower_bias: bfloat16 [16, 2048], P('peer', 'group'), may hold values from -5 to 5
- tower_head: bfloat16 [16, 2048], P('peer', 'group'), may hold values from -0.125 to 0.125
- head_bias: float32 [16], P('peer'), may hold values from -4 to 4
Outputs:
- predictions: float32 [98304, 16], P(('group', 'peer'))
The draws below stay inside these ranges and needn't reach their ends.
Inputs may be any that keep to these rules, and one draw needn't show every extreme that they name: `task_mask`: only bits 0 to 15 are used. Among the 384 samples of one device (aligned blocks of 384), at most 176 have any one bit set; in every run of 4 blocks that one group holds, some task's bit is set exactly 176 times in each block.
All inputs are finite; a program needn't handle non-finite values.
Results may differ from the reference program's by a relative error of at most 0.0003.
Values may be sent and summed in bfloat16 or wider, within the bound.
No kernel may reach another device: no remote copies, remote signals or barrier semaphores. Data moves between devices by JAX's collectives and lax.ppermute only.
A program may use at most 128 MiB of HBM per device.

```python
import jax
import jax.numpy as jnp
from jax import lax

D = 1024
H = 2048
CAP = 176
SAMP_DEV = 384
TASKS = 16
SAMPLES = 98304
N_PEER = 4


def draw_task_mask(key, part):
    blocks = SAMPLES // SAMP_DEV
    groups = blocks // N_PEER
    hot_task = jax.random.randint(jax.random.fold_in(key, 11), (groups,), 0, TASKS)
    active_block = jnp.repeat(hot_task, N_PEER)
    spread = jax.random.randint(jax.random.fold_in(key, 12), (blocks, TASKS), 0, CAP + 1)
    counts = spread * spread // CAP
    task_ids = jnp.arange(TASKS, dtype=jnp.int32)
    counts = jnp.where(task_ids[None, :] == active_block[:, None], CAP, counts)
    keys = jax.random.split(jax.random.fold_in(key, 13), blocks * TASKS)
    sort_orders = jax.vmap(lambda single: jax.random.permutation(single, SAMP_DEV))(keys)
    sort_orders = sort_orders.reshape(blocks, TASKS, SAMP_DEV).astype(jnp.int32)
    task_bits = (sort_orders < counts[:, :, None]).astype(jnp.int32)
    packed = jnp.sum(task_bits << task_ids[None, :, None], axis=1)
    return packed.reshape(-1).astype(jnp.int32)


def levels(own_key, dims, cuts, low, top_value):
    def one(dim, blocks):
        steps = jax.random.uniform(jax.random.fold_in(jax.random.fold_in(own_key, 6), dim), (blocks,), jnp.float32, low / len(cuts), top_value / len(cuts))
        return jnp.repeat(jnp.exp(steps), dims[dim] // blocks).reshape((-1,) + (1,) * (len(dims) - dim - 1))

    level = one(*cuts[0])
    for cut in cuts[1:]:
        level = level * one(*cut)
    return level


def scatter_about(stream_key, extent, scale, limit, pieces=(), held_as=jnp.bfloat16):
    gain = levels(stream_key, extent, pieces, -0.22, 0.18) if pieces else 1.0
    values = jax.random.normal(stream_key, extent, jnp.float32) * scale * gain
    return jnp.minimum(jnp.maximum(values, -limit), limit).astype(held_as)


def setup_inputs(seed: int = 0) -> dict:
    key_list = jax.random.split(jax.random.key(seed), 7)
    features = scatter_about(key_list[0], (SAMPLES, D), 1.0, 6.0, ((0, 256),))
    task_mask = draw_task_mask(jax.random.fold_in(key_list[6], 71), 0)
    tower_in = scatter_about(key_list[2], (TASKS, H, D), D ** -0.5, 0.1875, ((0, 4), (1, 64)))
    tower_bias = scatter_about(key_list[3], (TASKS, H), 1.0, 5.0, ((0, 4), (1, 64)))
    tower_head = scatter_about(key_list[4], (TASKS, H), H ** -0.5, 0.125, ((0, 4), (1, 64)))
    head_bias = scatter_about(key_list[5], (TASKS,), 1.0, 4.0, ((0, 4),), jnp.float32)
    return dict(features=features, task_mask=task_mask, tower_in=tower_in, tower_bias=tower_bias, tower_head=tower_head, head_bias=head_bias)


def block_logits(block_rows, block_mask, layer_entry, hidden_unit_bias, head_rows, out_bias):
    sample_count = block_rows.shape[0]
    task_ids = jnp.arange(TASKS, dtype=jnp.int32)
    task_bits = (block_mask[:, None] >> task_ids[None, :]) & 1
    inclusive = jnp.cumsum(task_bits, axis=0)
    slot_rank = inclusive - task_bits
    slot_indices = jnp.arange(CAP, dtype=jnp.int32)
    sample_index = jnp.sum((inclusive[:, :, None] <= slot_indices[None, None, :]).astype(jnp.int32), axis=0)
    sample_index = jnp.clip(sample_index, 0, sample_count - 1).astype(jnp.int32)
    gathered = block_rows.astype(jnp.float32)[sample_index]
    preact = jnp.einsum("tcd,thd->tch", gathered, layer_entry, precision=lax.Precision.HIGHEST)
    hidden = jnp.maximum(preact + hidden_unit_bias[:, None, :], 0.0)
    logit = jnp.sum(hidden * head_rows[:, None, :], axis=-1) + out_bias[:, None]
    picked = logit[task_ids[None, :], jnp.clip(slot_rank, 0, CAP - 1).astype(jnp.int32)]
    return jnp.where(task_bits == 1, picked, jnp.float32(0.0))


def reference(features, task_mask, tower_in, tower_bias, tower_head, head_bias):
    blocks = SAMPLES // SAMP_DEV
    layer_entry = tower_in.astype(jnp.float32)
    hidden_unit_bias = tower_bias.astype(jnp.float32)
    head_rows = tower_head.astype(jnp.float32)
    rows_blocked = features.reshape(blocks, SAMP_DEV, D)
    mask_blocked = task_mask.reshape(blocks, SAMP_DEV)

    def one_block(pair):
        return block_logits(pair[0], pair[1], layer_entry, hidden_unit_bias, head_rows, head_bias)

    result = lax.map(one_block, (rows_blocked, mask_blocked))
    return result.reshape(SAMPLES, TASKS)
```

```python
import functools

import jax
import jax.numpy as jnp
from jax import lax
from jax.experimental import pallas as pl
from jax.experimental.pallas import tpu as pltpu
from jax.sharding import PartitionSpec as P


Z, X, C = 8, 4, 2
HALF = 64
META = 8


def along_group(v, dz=0, dx=0, other_core=False):
    pairs = []
    for z in range(Z):
        for x in range(X):
            for c in range(C):
                to = (((z + dz) % Z) * X + (x + dx) % X) * C + (1 - c if other_core else c)
                pairs.append(((z * X + x) * C + c, to))
    return lax.ppermute(v, "group", pairs)


def along_peer(v, dy):
    n = lax.axis_size("peer")
    return lax.ppermute(v, "peer", [(i, (i + dy) % n) for i in range(n)])


def message(w, bias, head):
    row = jnp.concatenate([bias.reshape(1, HALF), head.reshape(1, HALF)], axis=1)
    meta = jnp.pad(row, ((0, META - 1), (0, w.shape[-1] - 2 * HALF)))
    return jnp.concatenate([w.reshape(HALF, w.shape[-1]), meta], axis=0)


def assembled(four):
    w = [m[:HALF] for m in four]
    meta = [m[HALF:] for m in four]
    row = jnp.concatenate(
        [m[:, :HALF] for m in meta] + [m[:, HALF : 2 * HALF] for m in meta], axis=1
    )
    row = jnp.pad(row, ((0, 0), (0, w[0].shape[1] - row.shape[1])))
    return jnp.concatenate([w[0], w[1], row, w[2], w[3]], axis=0)


N = 4 * HALF
TOP = N // 2 + META


def towers_kernel(blocks, pieces, last, *refs):
    nw = len(pieces)
    feats, refs = refs[:blocks], refs[blocks:]
    flat, refs = refs[: sum(pieces)], refs[sum(pieces) :]
    acc_in, refs = refs[0], refs[1:]
    out, x, w, meta, xsem, wsem = refs
    rows = feats[0].shape[0]
    half = N // 2
    copies = []
    k = 0
    for n, parts in enumerate(pieces):
        if parts == 1:
            q = flat[k]
            copies += [
                (q.at[pl.ds(0, half)], w.at[pl.ds(n * N, half)]),
                (q.at[pl.ds(half, META)], meta.at[pl.ds(n * META, META)]),
                (q.at[pl.ds(half + META, half)], w.at[pl.ds(n * N + half, half)]),
            ]
        else:
            top, bottom = flat[k], flat[k + 1]
            copies += [
                (top.at[pl.ds(0, half)], w.at[pl.ds(n * N, half)]),
                (top.at[pl.ds(half, META)], meta.at[pl.ds(n * META, META)]),
                (bottom.at[pl.ds(META, half)], w.at[pl.ds(n * N + half, half)]),
            ]
        k += parts
    wcopies = [pltpu.make_async_copy(a, b, wsem.at[i]) for i, (a, b) in enumerate(copies)]
    xcopies = [
        pltpu.make_async_copy(f, x.at[pl.ds(b * rows, rows)], xsem.at[b])
        for b, f in enumerate(feats)
    ]
    for c in wcopies:
        c.start()
    for c in xcopies:
        c.start()
    for c in wcopies:
        c.wait()

    def block(b, _):
        pltpu.make_async_copy(feats[0], x.at[pl.ds(b * rows, rows)], xsem.at[b]).wait()
        here = pl.ds(pl.multiple_of(b * rows, rows), rows)
        total = acc_in[here, :]
        for n in range(nw):
            p = lax.dot_general(
                x[here, :],
                w[pl.ds(n * N, N), :],
                (((1,), (1,)), ((), ())),
                preferred_element_type=jnp.float32,
            )
            both = meta[pl.ds(n * META, META), :].astype(jnp.float32)
            h = jnp.maximum(p + both[0:1, :N], 0.0) * both[0:1, N : 2 * N]
            total = total + (h[:, : N // 2] + h[:, N // 2 :])
        if last:
            lane = lax.broadcasted_iota(jnp.int32, (8, N // 2), 1)
            tower = lax.broadcasted_iota(jnp.int32, (8, N // 2), 0)
            pick = (((lane % HALF) // (HALF // 4)) == tower).astype(jnp.float32)
            out[b] = lax.dot_general(
                pick,
                total,
                (((1,), (1,)), ((), ())),
                precision=lax.Precision.HIGHEST,
                preferred_element_type=jnp.float32,
            )
        else:
            out[here, :] = total
        return 0

    lax.fori_loop(0, blocks, block, 0)


def towers(feats, groups, acc, last=False):
    blocks, rows, depth = len(feats), *feats[0].shape
    pieces = tuple(len(g) for g in groups)
    flat = [m for g in groups for m in g]
    nw = len(groups)
    size = blocks * rows
    if last:
        out = jax.ShapeDtypeStruct((blocks, 8, rows), jnp.float32)
    else:
        out = jax.ShapeDtypeStruct(acc.shape, jnp.float32)
    any_ = pl.BlockSpec(memory_space=pl.ANY)
    vmem = pl.BlockSpec(memory_space=pltpu.VMEM)
    return pl.pallas_call(
        functools.partial(towers_kernel, blocks, pieces, last),
        out_shape=out,
        in_specs=[any_] * (blocks + len(flat)) + [vmem],
        out_specs=vmem,
        scratch_shapes=[
            pltpu.VMEM((size, depth), jnp.bfloat16),
            pltpu.VMEM((nw * N, depth), jnp.bfloat16),
            pltpu.VMEM((nw * META, depth), jnp.bfloat16),
            pltpu.SemaphoreType.DMA((blocks,)),
            pltpu.SemaphoreType.DMA((3 * nw,)),
        ],
        compiler_params=pltpu.CompilerParams(vmem_limit_bytes=24 * 2**20),
        cost_estimate=pl.CostEstimate(
            flops=2 * size * nw * N * depth,
            bytes_accessed=2 * depth * (size + nw * N),
            transcendentals=0,
        ),
    )(*feats, *flat, acc)


def shards(features, task_mask, tower_in, tower_bias, tower_head, head_bias):
    half = tower_in.shape[1] // 2
    a0 = message(tower_in[:, :half], tower_bias[:, :half], tower_head[:, :half])
    b0 = message(tower_in[:, half:], tower_bias[:, half:], tower_head[:, half:])

    ax = [a0, along_group(a0, dx=1), along_group(a0, dx=-1), along_group(a0, dx=2)]
    bp, bm = [b0], [b0]
    for _ in range(3):
        bp.append(along_group(bp[-1], dz=1))
        bm.append(along_group(bm[-1], dz=-1))
    b4 = along_group(bp[3], dz=1)

    qa = assembled(ax)
    ap, am = [qa], [qa]
    for _ in range(3):
        ap.append(along_group(ap[-1], dz=1))
        am.append(along_group(am[-1], dz=-1))
    a4 = (along_group(ap[3][:TOP], dz=1), along_group(am[3][N // 2 :], dz=-1))

    def over_x(q):
        p, m = along_group(q, dx=1), along_group(q, dx=-1)
        return p, m, (along_group(p[:TOP], dx=1), along_group(m[N // 2 :], dx=-1))

    q1 = assembled([b0, bp[1], bm[1], bp[2]])
    q2 = assembled([bm[2], bp[3], bm[3], b4])
    q1p, q1m, q1h = over_x(q1)
    q2p, q2m, q2h = over_x(q2)

    rows = features.shape[0]
    fp, fm = along_peer(features, 1), along_peer(features, -1)
    f2 = jnp.concatenate(
        [along_peer(fp[: rows // 2], 1), along_peer(fm[rows // 2 :], -1)], axis=0
    )
    feats = []
    for f in (features, fp, fm, f2):
        feats += [f, along_group(f, other_core=True)]

    acc = jnp.zeros((len(feats) * rows, N // 2), jnp.float32)
    acc = towers(feats, [(qa,), (q1,), (ap[1],), (am[1],), (q2,), (q1p,), (q1m,)], acc)
    acc = towers(feats, [(ap[2],), (am[2],), (q2p,), (q2m,), q1h], acc)
    acc = towers(feats, [(ap[3],), (am[3],), q2h], acc)
    part = towers(feats, [a4], acc, last=True)[:, :4]

    here, there = part[0::2], part[1::2]
    full = here + along_group(there, other_core=True) + head_bias[None, :, None]
    back = [
        full[0],
        along_peer(full[1], -1),
        along_peer(full[3], 2),
        along_peer(full[2], 1),
    ]
    y = lax.axis_index("peer")
    n = len(back)
    logits = lax.dynamic_slice_in_dim(jnp.stack(back + back), (n - y) % n, n, 0)
    logits = logits.reshape(-1, rows)
    bits = task_mask[None, :] >> jnp.arange(logits.shape[0], dtype=jnp.int32)[:, None] & 1
    return jnp.where(bits == 1, logits, 0.0).T


def solution(mesh):
    placed = (
        P(("group", "peer"), None),
        P(("group", "peer")),
        P("peer", "group", None),
        P("peer", "group"),
        P("peer", "group"),
        P("peer"),
    )
    return jax.shard_map(
        shards, mesh=mesh, in_specs=placed, out_specs=P(("group", "peer"), None), check_vma=False
    )
```

```python
import functools

import jax
import jax.numpy as jnp
from jax import lax
from jax.experimental import pallas as pl
from jax.experimental.pallas import tpu as pltpu
from jax.sharding import PartitionSpec as P


Z, X, C = 8, 4, 2
HALF = 64
META = 8
N = 4 * HALF
ANY = pl.BlockSpec(memory_space=pl.ANY)
HBM = pl.BlockSpec(memory_space=pltpu.HBM)
VMEM = pl.BlockSpec(memory_space=pltpu.VMEM)


def along_group(v, plus, minus=None):
    pairs = []
    for z in range(Z):
        for x in range(X):
            for c in range(C):
                dz, dx, dc = minus if minus is not None and c else plus
                to = (((z + dz) % Z) * X + (x + dx) % X) * C + (c + dc) % C
                pairs.append(((z * X + x) * C + c, to))
    return lax.ppermute(v, "group", pairs)


def along_peer(v, dy):
    n = lax.axis_size("peer")
    return lax.ppermute(v, "peer", [(i, (i + dy) % n) for i in range(n)])


def along_peer_by_core(v):
    g, n = lax.axis_size("group"), lax.axis_size("peer")
    pairs = [
        (i * n + j, i * n + (j + (-1 if i % C else 1)) % n) for i in range(g) for j in range(n)
    ]
    return lax.ppermute(v, ("group", "peer"), pairs)


def split_kernel(w, both_in, a, b, both, sem):
    t, h, d = w.shape
    q = h // 2
    small = [pltpu.make_async_copy(both_in, both, sem.at[2 * t])]
    copies = []
    for i in range(t):
        copies.append(pltpu.make_async_copy(w.at[i, pl.ds(0, q)], a.at[pl.ds(i * q, q)], sem.at[2 * i]))
        copies.append(
            pltpu.make_async_copy(w.at[i, pl.ds(q, q)], b.at[pl.ds(i * q, q)], sem.at[2 * i + 1])
        )
    for c in small + copies:
        c.start()
    for c in small:
        c.wait()
    unit = lax.broadcasted_iota(jnp.int32, (h, t * 128), 0)
    lane = lax.broadcasted_iota(jnp.int32, (h, t * 128), 1)
    for part, out in enumerate((a, b)):
        row = jnp.zeros((1, 128), jnp.float32)
        for k in range(2):
            place = (lane % 128 == k * HALF + (lane // 128) * q + unit - part * q) & (unit // q == part)
            moved = jnp.dot(
                both[...], place.astype(jnp.bfloat16), preferred_element_type=jnp.float32
            )
            for i in range(t):
                row = row + moved[k * t + i : k * t + i + 1, i * 128 : (i + 1) * 128]
        first = lax.broadcasted_iota(jnp.int32, (META, 128), 0) == 0
        out[pl.ds(HALF, META), :128] = jnp.where(first, row, 0.0).astype(jnp.bfloat16)
        out[pl.ds(HALF, META), 128:] = jnp.zeros((META, d - 128), jnp.bfloat16)
    for c in copies:
        c.wait()


def split(w, bias, head):
    shape = jax.ShapeDtypeStruct((HALF + META, w.shape[2]), w.dtype)
    return pl.pallas_call(
        split_kernel,
        out_shape=(shape, shape),
        in_specs=[HBM] * 2,
        out_specs=(VMEM, VMEM),
        scratch_shapes=[
            pltpu.VMEM((2 * w.shape[0], w.shape[1]), bias.dtype),
            pltpu.SemaphoreType.DMA((2 * w.shape[0] + 1,)),
        ],
        compiler_params=pltpu.CompilerParams(vmem_limit_bytes=4 * 2**20),
    )(w, jnp.concatenate([bias, head], axis=0))


def assemble_kernel(after, *refs):
    four, out, metas, sem = refs[:4], refs[4 + after], refs[5 + after], refs[6 + after]
    at = (0, HALF, N // 2 + META, N // 2 + META + HALF)
    copies = []
    for i, m in enumerate(four):
        copies.append(
            pltpu.make_async_copy(m.at[pl.ds(HALF, META)], metas.at[pl.ds(i * META, META)], sem.at[i])
        )
    for i, m in enumerate(four):
        copies.append(
            pltpu.make_async_copy(m.at[pl.ds(0, HALF)], out.at[pl.ds(at[i], HALF)], sem.at[4 + i])
        )
    for c in copies:
        c.start()
    for c in copies[:4]:
        c.wait()
    rows = [metas[pl.ds(i * META, META), :128].astype(jnp.float32) for i in range(4)]
    turned = [pltpu.roll(r, HALF, 1) for r in rows]
    low = lax.broadcasted_iota(jnp.int32, (META, 128), 1) < HALF
    tiles = [
        jnp.where(low, rows[0], turned[1]),
        jnp.where(low, rows[2], turned[3]),
        jnp.where(low, turned[0], rows[1]),
        jnp.where(low, turned[2], rows[3]),
    ]
    here = pl.ds(N // 2, META)
    for i, tile in enumerate(tiles):
        out[here, i * 128 : (i + 1) * 128] = tile.astype(jnp.bfloat16)
    out[here, 512:] = jnp.zeros((META, out.shape[1] - 512), jnp.bfloat16)
    for c in copies[4:]:
        c.wait()


def assembled(four, after=()):
    d = four[0].shape[1]
    return pl.pallas_call(
        functools.partial(assemble_kernel, len(after)),
        out_shape=jax.ShapeDtypeStruct((N + META, d), four[0].dtype),
        in_specs=[ANY] * (4 + len(after)),
        out_specs=VMEM,
        scratch_shapes=[pltpu.VMEM((4 * META, d), jnp.bfloat16), pltpu.SemaphoreType.DMA((8,))],
        compiler_params=pltpu.CompilerParams(vmem_limit_bytes=4 * 2**20),
    )(*four, *after)


STEP = 384


def towers_kernel(nfeats, nw, per, span, given, last, *refs):
    lo, hi = span
    feats, refs = refs[:nfeats], refs[nfeats:]
    flat, refs = refs[:nw], refs[nw:]
    if given:
        x, acc_in, refs = refs[0], refs[1], refs[2:]
    if nfeats:
        x, refs = refs[0], refs[1:]
    acc, refs = refs[0], refs[1:]
    if last:
        part, refs = refs[0], refs[1:]
    (xsem,) = refs
    half = N // 2
    copies = [
        pltpu.make_async_copy(f, x.at[pl.ds(lo + b * STEP, STEP)], xsem.at[b])
        for b, f in enumerate(feats)
    ]
    for c in copies:
        c.start()

    def step(i, _):
        if nfeats:
            for k in range(per):
                b = i * per + k
                rows = pl.ds(pl.multiple_of(lo + b * STEP, STEP), STEP)
                pltpu.make_async_copy(feats[0], x.at[rows], xsem.at[b]).wait()
        heres = [
            pl.ds(pl.multiple_of(lo + (i * per + k) * STEP, STEP), STEP) for k in range(per)
        ]
        totals = [None if nfeats else acc_in[here, :] for here in heres]
        for q in flat:
            w = jnp.concatenate([q[:half], q[half + META : N + META]], axis=0)
            both = q[half : half + META, : 2 * N].astype(jnp.float32)
            for k, here in enumerate(heres):
                p = lax.dot_general(
                    x[here, :], w, (((1,), (1,)), ((), ())), preferred_element_type=jnp.float32
                )
                h = jnp.maximum(p + both[0:1, :N], 0.0) * both[0:1, N:]
                h = h[:, :half] + h[:, half:]
                totals[k] = h if totals[k] is None else totals[k] + h
        for k, here in enumerate(heres):
            if last:
                turned = totals[k].T
                r = HALF // 4
                for t in range(4):
                    mine = turned[t * r : (t + 1) * r] + turned[HALF + t * r : HALF + (t + 1) * r]
                    part[i * per + k, pl.ds(t, 1), :] = jnp.sum(mine, axis=0, keepdims=True)
            else:
                acc[here, :] = totals[k]
        return 0

    lax.fori_loop(0, (hi - lo) // (per * STEP), step, 0)


def towers(messages, per, feats=(), rows=None, span=None, x=None, acc=None, last=False):
    nw, d = len(messages), messages[0].shape[1]
    given = x is not None
    span = span or (0, rows)
    nf = len(feats)
    xs = jax.ShapeDtypeStruct((rows, d), jnp.bfloat16)
    sums = jax.ShapeDtypeStruct((rows, N // 2), jnp.float32)
    out = ((xs,) if nf else ()) + (sums,)
    alias = {}
    if given:
        alias = {nf + nw: 0, nf + nw + 1: 1} if nf else {nf + nw + 1: 0}
    if last:
        out += (jax.ShapeDtypeStruct((rows // STEP, 4, STEP), jnp.float32),)
    size = span[1] - span[0]
    return pl.pallas_call(
        functools.partial(towers_kernel, nf, nw, per, span, given, last),
        out_shape=out,
        in_specs=[ANY] * nf + [VMEM] * (nw + 2 * given),
        out_specs=(VMEM,) * len(out),
        input_output_aliases=alias,
        scratch_shapes=[pltpu.SemaphoreType.DMA((max(nf, 1),))],
        compiler_params=pltpu.CompilerParams(vmem_limit_bytes=24 * 2**20),
        cost_estimate=pl.CostEstimate(
            flops=2 * size * nw * N * d, bytes_accessed=2 * d * (size + nw * N), transcendentals=0
        ),
    )(*feats, *messages, *((x, acc) if given else ()))


def predictions(features, task_mask, tower_in, tower_bias, tower_head, head_bias):
    first = lax.axis_index("group") % C == 0

    def by_core(one, two):
        return jnp.where(first, one, two)

    a0, b0 = split(tower_in, tower_bias, tower_head)

    bp, bm = [b0], [b0]
    for _ in range(3):
        bp.append(along_group(bp[-1], (1, 0, 0)))
        bm.append(along_group(bm[-1], (-1, 0, 0)))
    b4 = along_group(by_core(bp[3], bm[3]), (1, 0, 0), (-1, 0, 0))

    ax = [a0, along_group(a0, (0, 1, 0)), along_group(a0, (0, -1, 0)), along_group(a0, (0, 2, 0))]
    qa = assembled(ax)
    ap, am = [qa], [qa]
    for _ in range(3):
        ap.append(along_group(ap[-1], (1, 0, 0)))
        am.append(along_group(am[-1], (-1, 0, 0)))
    a4 = along_group(by_core(ap[3], am[3]), (1, 0, 0), (-1, 0, 0))

    def over_x(four):
        q = assembled(four)
        p = along_group(q, (0, 1, 0))
        m = along_group(q, (0, -1, 0))
        return q, p, m, along_group(by_core(p, m), (0, 1, 0), (0, -1, 0))

    q1, q1p, q1m, q1h = over_x([b0, bp[1], bm[1], bp[2]])
    q2, q2p, q2m, q2h = over_x([bm[2], bp[3], bm[3], b4])

    fp, fm = along_peer(features, 1), along_peer(features, -1)
    f2 = along_peer_by_core(by_core(fp, fm))
    other = (0, 0, 1)
    near = [features, along_group(features, other), fp, along_group(fp, other)]
    near += [fm, along_group(fm, other)]
    far = [f2, along_group(f2, other)]

    rows = features.shape[0]
    size = (len(near) + len(far)) * rows
    mid = len(near) * rows
    x, acc = towers([qa, q1], 2, near, size, (0, mid))
    (acc,) = towers([ap[1], am[1], q1p, q1m], 2, (), size, (0, mid), x, acc)
    early = [qa, q1, ap[1], am[1], q1p, q1m]
    x, acc = towers(early, 1, far, size, (mid, size), x, acc)
    (acc,) = towers([ap[2], am[2], q1h, q2], 4, (), size, None, x, acc)
    (acc,) = towers([q2p, q2m, ap[3], am[3]], 4, (), size, None, x, acc)
    _, part = towers([a4, q2h], 4, (), size, None, x, acc, last=True)

    full = part[0::2] + along_group(part[1::2], other) + head_bias[None, :, None]
    back = [full[0], along_peer(full[1], -1), along_peer(full[3], 2), along_peer(full[2], 1)]
    y = lax.axis_index("peer")
    n = len(back)
    logits = lax.dynamic_slice_in_dim(jnp.stack(back + back), (n - y) % n, n, 0)
    logits = logits.reshape(-1, rows)
    bits = task_mask[None, :] >> jnp.arange(logits.shape[0], dtype=jnp.int32)[:, None] & 1
    return jnp.where(bits == 1, logits, 0.0).T


def solution(mesh):
    placed = (
        P(("group", "peer"), None),
        P(("group", "peer")),
        P("peer", "group", None),
        P("peer", "group"),
        P("peer", "group"),
        P("peer"),
    )
    return jax.shard_map(predictions, mesh=mesh, in_specs=placed, out_specs=P(("group", "peer"), None), check_vma=False)
```
